16 devices in a mesh: rep: 1, r: 4 (over y, z), s: 4 (over x, core).
Axes of the slice: x: 2, y: 2, z: 2, core: 2. Of those that a mesh axis runs over, the one named last changes fastest.
Arguments:
- x: bfloat16 [16, 4096, 1024], P(('rep', 'r', 's'))
- dy: bfloat16 [16, 4096, 1024], P(('rep', 'r', 's'))
- w_gate: bfloat16 [2, 1024, 2816], P(None, 's')
- w_up: bfloat16 [2, 1024, 2816], P(None, 's')
- w_down: bfloat16 [2, 2816, 1024], P(None, 's')
- m_w_gate: float32 [2, 1024, 2816], P(None, 's')
- m_w_up: float32 [2, 1024, 2816], P(None, 's')
- m_w_down: float32 [2, 2816, 1024], P(None, 's')
- v_w_gate: float32 [2, 1024, 2816], P(None, 's')
- v_w_up: float32 [2, 1024, 2816], P(None, 's')
- v_w_down: float32 [2, 2816, 1024], P(None, 's')
Outputs:
- output 1: bfloat16 [2, 1024, 2816], P('rep', 's')
- output 2: bfloat16 [2, 1024, 2816], P('rep', 's')
- output 3: bfloat16 [2, 2816, 1024], P('rep', 's')
- output 4: float32 [2, 1024, 2816], P('rep', 's')
- output 5: float32 [2, 1024, 2816], P('rep', 's')
- output 6: float32 [2, 2816, 1024], P('rep', 's')
- output 7: float32 [2, 1024, 2816], P('rep', 's')
- output 8: float32 [2, 1024, 2816], P('rep', 's')
- output 9: float32 [2, 2816, 1024], P('rep', 's')
All inputs are finite; a program needn't handle non-finite values.
Results may differ from the reference program's by a relative error of at most 0.02.
Values are sent between devices in bfloat16 or wider.
A program may use at most 2 GiB of HBM per device.

```python
import jax
import jax.numpy as jnp
from jax import lax

SEQUENCES = 16
TOKENS = 4096
D = 1024
FF = 2816
LAYERS = 2
NAMES = ("w_gate", "w_up", "w_down")
SHAPES = {"w_gate": (LAYERS, D, FF), "w_up": (LAYERS, D, FF), "w_down": (LAYERS, FF, D)}


def bump(key, n, height):
    away = (jnp.arange(n, dtype=jnp.int32) - jax.random.randint(key, (), 0, n, jnp.int32)) % n
    return jnp.where(away < n // 8, height, 1.0)


def together(key, own, strength):
    shared = jax.random.normal(key, own.shape[1:], jnp.float32)
    return (own + strength * shared) * lax.rsqrt(1 + strength * strength)


def setup_inputs(seed: int = 0, part: int = 0) -> dict:
    kx, kdy, ka, kb, kz, kf, kh, kl, *keys = jax.random.split(jax.random.key(seed), 8 + 3 * len(NAMES))
    kx, kdy, ka, kb = (jax.random.fold_in(k, part) for k in (kx, kdy, ka, kb))
    kw, km, kv = (keys[i::3] for i in range(3))
    shape = (SEQUENCES, TOKENS, D)
    much_x, much_dy = jax.random.uniform(kz, (2,), jnp.float32, 0.0, 1.0)
    loud = 2.0 ** jax.random.uniform(jax.random.fold_in(kz, 1), (), jnp.float32, -1.0, 2.0)
    layers = 2.0 ** jax.random.uniform(kl, (LAYERS, 1, 1), jnp.float32, -1.0, 1.0)
    x = together(ka, jax.random.normal(kx, shape, jnp.float32), much_x) * bump(kf, D, 4.0)
    dy = together(kb, jax.random.normal(kdy, shape, jnp.float32), much_dy)
    drawn = {"x": x.astype(jnp.bfloat16), "dy": (loud * dy * (SEQUENCES * TOKENS) ** -0.5).astype(jnp.bfloat16)}
    for key, name in zip(kw, NAMES, strict=True):
        w = jax.random.normal(key, SHAPES[name], jnp.float32) * SHAPES[name][1] ** -0.5
        drawn[name] = (w * {"w_gate": 1.0, "w_up": bump(kh, FF, 4.0), "w_down": layers}[name]).astype(jnp.bfloat16)
    for key, name in zip(km, NAMES, strict=True):
        drawn[f"m_{name}"] = 0.1 * jax.random.normal(key, SHAPES[name], jnp.float32)
    for key, name in zip(kv, NAMES, strict=True):
        drawn[f"v_{name}"] = jax.random.uniform(key, SHAPES[name], jnp.float32, 0.005, 0.015)
    return drawn


def matmul(a, w):
    return jnp.dot(a, w, preferred_element_type=jnp.float32).astype(jnp.bfloat16)


def normed(h):
    wide = h.astype(jnp.float32)
    scale = lax.rsqrt(jnp.mean(wide**2, -1, keepdims=True) + 1e-6)
    return (wide * scale).astype(jnp.bfloat16)


def layer(h, w):
    a = normed(h)
    gate = jnp.dot(a, w["w_gate"], preferred_element_type=jnp.float32)
    up = jnp.dot(a, w["w_up"], preferred_element_type=jnp.float32)
    return h + matmul((jax.nn.silu(gate) * up).astype(jnp.bfloat16), w["w_down"])


def adamw(w, m, v, g):
    m = 0.9 * m + 0.1 * g
    v = 0.95 * v + 0.05 * g * g
    step = m * lax.rsqrt(v + 1e-8) + 0.1 * w
    return (w - 0.02 * step).astype(jnp.bfloat16), m, v


def stack(weights, h):
    return lax.scan(lambda h, w: (layer(h, w), None), h, weights)[0]


def reference(x, dy, w_gate, w_up, w_down, m_w_gate, m_w_up, m_w_down, v_w_gate, v_w_up, v_w_down):
    weights = dict(zip(NAMES, (w_gate, w_up, w_down), strict=True))

    def take(so_far, sequence):
        h, by_y = sequence
        _, back = jax.vjp(lambda w: stack(w, h), weights)
        return jax.tree.map(lambda total, term: total + term.astype(jnp.float32), so_far, back(by_y)[0]), None

    none_yet = {name: jnp.zeros(w.shape, jnp.float32) for name, w in weights.items()}
    by_weights, _ = lax.scan(take, none_yet, (x, dy))
    gradients = [by_weights[name].astype(jnp.bfloat16).astype(jnp.float32) for name in NAMES]
    new = [
        adamw(w.astype(jnp.float32), m, v, g)
        for w, m, v, g in zip((w_gate, w_up, w_down), (m_w_gate, m_w_up, m_w_down), (v_w_gate, v_w_up, v_w_down), gradients, strict=True)
    ]
    return tuple(one[which] for which in range(3) for one in new)
```

```python
import functools

import jax
import jax.numpy as jnp
from jax import lax
from jax.experimental import pallas as pl
from jax.experimental.pallas import tpu as pltpu
from jax.sharding import PartitionSpec as P

NAMES = ("w_gate", "w_up", "w_down")
BF, F32 = jnp.bfloat16, jnp.float32
MESH = pl.DeviceIdType.MESH
NN, TB, TA = ((((1,), (0,)), ((), ())), (((1,), (1,)), ((), ())), (((0,), (0,)), ((), ())))
VMEM = 60 * 2**20


def dot(a, b, dims):
    return lax.dot_general(a, b, dims, preferred_element_type=F32)


def whole(w):
    return jnp.concatenate([w[s] for s in range(4)], axis=1)


def scale_of(wide):
    return lax.rsqrt(jnp.mean(wide * wide, -1, keepdims=True) + 1e-6)


def normed(h):
    wide = h.astype(F32)
    return (wide * scale_of(wide)).astype(BF)


def adamw(w, m, v, g):
    m = 0.9 * m + 0.1 * g
    v = 0.95 * v + 0.05 * g * g
    step = m * lax.rsqrt(v + 1e-8) + 0.1 * w
    return (w - 0.02 * step).astype(BF), m, v


def params(axes, **more):
    return pltpu.CompilerParams(dimension_semantics=("arbitrary",) * axes, vmem_limit_bytes=VMEM, **more)


def cost(flops, bytes_):
    return pl.CostEstimate(flops=flops, bytes_accessed=bytes_, transcendentals=0)


def hidden(a, wg, wu, tm=512, tn=1408):
    tokens, d = a.shape
    n = wg.shape[1]

    def kernel(a, g, u, o):
        gate, up = dot(a[...], whole(g), TB), dot(a[...], whole(u), TB)
        o[...] = (gate * jax.nn.sigmoid(gate) * up).astype(BF)

    w = pl.BlockSpec((4, tn, d // 4), lambda n, m: (0, n, 0))
    return pl.pallas_call(
        kernel,
        out_shape=jax.ShapeDtypeStruct((tokens, n), BF),
        grid=(n // tn, tokens // tm),
        in_specs=[pl.BlockSpec((tm, d), lambda n, m: (m, 0)), w, w],
        out_specs=pl.BlockSpec((tm, tn), lambda n, m: (m, n)),
        compiler_params=params(2),
        cost_estimate=cost(4 * tokens * d * n, 2 * tokens * (d + n)),
        name="hidden",
    )(a, wg, wu)


def down(p, wd, h, tm=512):
    tokens, n = p.shape
    d = h.shape[1]

    def kernel(p, w, h, ho, ao):
        new = h[...] + dot(p[...], w[...], NN).astype(BF)
        ho[...] = new
        ao[...] = normed(new)

    row = pl.BlockSpec((tm, d), lambda m: (m, 0))
    return pl.pallas_call(
        kernel,
        out_shape=(jax.ShapeDtypeStruct((tokens, d), BF),) * 2,
        grid=(tokens // tm,),
        in_specs=[pl.BlockSpec((tm, n), lambda m: (m, 0)), pl.BlockSpec((n, d), lambda m: (0, 0)), row],
        out_specs=(row, row),
        compiler_params=params(1),
        cost_estimate=cost(2 * tokens * d * n, 2 * tokens * (3 * d + n)),
        name="down",
    )(p, wd, h)


def inner(a, dy, wg, wu, wd, tm=512, tn=704):
    tokens, d = a.shape
    n = wd.shape[0]

    def kernel(a, dy, g, u, w, o):
        gate, up = dot(whole(g), a[...], TB), dot(whole(u), a[...], TB)
        by_p = dot(w[...], dy[...], TB).astype(BF).astype(F32)
        sig = jax.nn.sigmoid(gate)
        act = gate * sig
        o[0] = (act * up).astype(BF)
        o[1] = (by_p * up * (sig * (1.0 + gate * (1.0 - sig)))).astype(BF)
        o[2] = (by_p * act).astype(BF)

    w = pl.BlockSpec((4, tn, d // 4), lambda n, m: (0, n, 0))
    act = pl.BlockSpec((tm, d), lambda n, m: (m, 0))
    return pl.pallas_call(
        kernel,
        out_shape=jax.ShapeDtypeStruct((3, n, tokens), BF),
        grid=(n // tn, tokens // tm),
        in_specs=[act, act, w, w, pl.BlockSpec((tn, d), lambda n, m: (n, 0))],
        out_specs=pl.BlockSpec((3, tn, tm), lambda n, m: (0, n, m)),
        compiler_params=params(2),
        cost_estimate=cost(6 * tokens * d * n, 2 * tokens * (2 * d + 3 * n)),
        name="inner",
    )(a, dy, wg, wu, wd)


def below(x, wg, wu, h, dh, tm=256):
    tokens, d = h.shape
    n = x.shape[1]

    def kernel(x, g, u, h, dh, o):
        by_a = dot(x[0], whole(g), TA).astype(BF).astype(F32) + dot(x[1], whole(u), TA).astype(BF).astype(F32)
        wide = h[...].astype(F32)
        r = scale_of(wide)
        by_h = by_a * r - wide * (r * r * r) * jnp.mean(by_a * wide, -1, keepdims=True)
        o[...] = dh[...] + by_h.astype(BF)

    row = pl.BlockSpec((tm, d), lambda m: (m, 0))
    w = pl.BlockSpec((4, n, d // 4), lambda m: (0, 0, 0))

    def two(x_gate, x_up, g, u, h, dh, o):
        kernel((x_gate[0], x_up[0]), g, u, h, dh, o)

    return pl.pallas_call(
        two,
        out_shape=jax.ShapeDtypeStruct((tokens, d), BF),
        grid=(tokens // tm,),
        in_specs=[pl.BlockSpec((1, n, tm), lambda m: (1, 0, m)), pl.BlockSpec((1, n, tm), lambda m: (2, 0, m)), w, w, row, row],
        out_specs=row,
        compiler_params=params(1),
        cost_estimate=cost(4 * tokens * d * n, 2 * tokens * (3 * d + 2 * n)),
        name="below",
    )(x, x, wg, wu, h, dh)


LAG = (0, 1, 3, 5, 7)
ROWS = 64


def summed(xs, rights):
    _, n, tokens = xs[0].shape
    d = rights[0][0].shape[1]
    quarter = n // 4
    per = quarter // ROWS
    layers = len(xs)
    chunks = layers * 3 * per
    wide = d // 4
    slots = 4

    def kernel(*refs):
        x_refs, r_refs = refs[:layers], refs[layers : 3 * layers]
        out, right, acc, csend, crecv, mine, xsend, xrecv, ysend, yrecv, zsend, zrecv, rsem, csems, xsems, ysems, zsems = refs[3 * layers :]
        t = pl.program_id(0)
        s, r = lax.axis_index("s"), lax.axis_index("r")
        core, x, y, z = s % 2, s // 2, r // 2, r % 2
        other, over_x, over_y, over_z = s + 1 - 2 * core, s + 2 - 4 * x, r + 2 - 4 * y, r + 1 - 2 * z

        def load(i):
            return pltpu.make_async_copy(r_refs[i], right.at[i % 2], rsem.at[i % 2])

        def send(src, dst, sems, slot, to):
            return pltpu.make_async_remote_copy(
                src_ref=src.at[slot], dst_ref=dst.at[slot], send_sem=sems.at[0, slot], recv_sem=sems.at[1, slot],
                device_id=to, device_id_type=MESH,
            )

        def along_core(u):
            return send(csend, crecv, csems, u % 2, {"s": other})

        def along_x(u):
            return send(xsend, xrecv, xsems, u % slots, {"s": over_x})

        def along_y(u):
            return send(ysend, yrecv, ysems, u % slots, {"r": over_y})

        def along_z(u):
            return send(zsend, zrecv, zsems, u % slots, {"r": over_z})

        @pl.when(t == 0)
        def _():
            load(0).start()
            load(1).start()
            barrier = pltpu.get_barrier_semaphore()
            for to in ({"s": other}, {"s": over_x}, {"r": over_y}, {"r": over_z}):
                pl.semaphore_signal(barrier, inc=1, device_id=to, device_id_type=MESH)
            pl.semaphore_wait(barrier, 4)

        for layer in range(layers):
            first = layer * 3 * per

            @pl.when(t == first)
            def _():
                load(2 * layer).wait()
                if layer:
                    load(2 * layer + 1).start()

            @pl.when(t == first + per)
            def _():
                load(2 * layer + 1).wait()
                if layer + 1 < layers:
                    load(2 * layer + 2).start()

            @pl.when((t >= first) & (t < first + per))
            def _():
                o = dot(x_refs[layer][...].reshape(4 * ROWS, tokens), right[0], NN)
                for q in range(4):
                    acc[t % 2, q] = o[ROWS * q : ROWS * (q + 1)]

            @pl.when((t >= first + per) & (t < first + 3 * per))
            def _():
                o = dot(x_refs[layer][...].reshape(4 * ROWS, tokens), right[1], NN)
                for q in range(4):
                    for p in range(4):
                        acc[t % 2, p, :, wide * q : wide * (q + 1)] = o[ROWS * q : ROWS * (q + 1), wide * p : wide * (p + 1)]

        @pl.when(t >= LAG[4])
        def _():
            u = t - LAG[4]
            along_z(u).wait()
            out[0] = (zsend[u % slots].astype(F32) + zrecv[u % slots].astype(F32)).astype(BF)

        @pl.when((t >= LAG[3]) & (t < chunks + LAG[3]))
        def _():
            u = t - LAG[3]
            along_y(u).wait()
            zsend[u % slots] = (ysend[u % slots].astype(F32) + yrecv[u % slots].astype(F32)).astype(BF)
            along_z(u).start()

        @pl.when((t >= LAG[2]) & (t < chunks + LAG[2]))
        def _():
            u = t - LAG[2]
            along_x(u).wait()
            ysend[u % slots] = (mine[u % slots] + xrecv[u % slots].astype(F32)).astype(BF)
            along_y(u).start()

        @pl.when((t >= LAG[1]) & (t < chunks + LAG[1]))
        def _():
            u = t - LAG[1]
            along_core(u).wait()
            xsend[u % slots] = (acc[u % 2, 2 - 2 * x + core] + crecv[u % 2, 1 - x].astype(F32)).astype(BF)
            along_x(u).start()
            mine[u % slots] = acc[u % 2, 2 * x + core] + crecv[u % 2, x].astype(F32)

        @pl.when(t < chunks)
        def _():
            for j in range(2):
                csend[t % 2, j] = acc[t % 2, 2 * j + 1 - core].astype(BF)
            along_core(t).start()

    def lhs(layer):
        def index(t):
            u = jnp.clip(t - layer * 3 * per, 0, 3 * per - 1)
            return u // per, 0, u % per, 0

        return pl.BlockSpec((1, 4, ROWS, tokens), index)

    block = (ROWS, d)
    dma = pltpu.SemaphoreType.DMA
    return pl.pallas_call(
        kernel,
        out_shape=jax.ShapeDtypeStruct((chunks,) + block, BF),
        grid=(chunks + LAG[4],),
        in_specs=[lhs(layer) for layer in range(layers)] + [pl.BlockSpec(memory_space=pl.ANY)] * (2 * layers),
        out_specs=pl.BlockSpec((1,) + block, lambda t: (jnp.maximum(t - LAG[4], 0), 0, 0)),
        scratch_shapes=[
            pltpu.VMEM((2, tokens, d), BF),
            pltpu.VMEM((2, 4) + block, F32),
            pltpu.VMEM((2, 2) + block, BF),
            pltpu.VMEM((2, 2) + block, BF),
            pltpu.VMEM((slots,) + block, F32),
        ]
        + [pltpu.VMEM((slots,) + block, BF)] * 6
        + [dma((2,)), dma((2, 2)), dma((2, slots)), dma((2, slots)), dma((2, slots))],
        compiler_params=params(1, collective_id=0, has_side_effects=True),
        cost_estimate=cost(2 * chunks * 4 * ROWS * tokens * d, 2 * layers * tokens * (3 * n + 2 * d)),
        name="summed",
    )(*[x.reshape(3, 4, quarter, tokens) for x in xs], *[r for pair in rights for r in pair])


def solution(mesh):
    def step(x, dy, *arrays):
        weights, m, v = (arrays[i : i + 3] for i in (0, 3, 6))
        layers = weights[0].shape[0]

        def fetched(number):
            gate, up = (lax.all_gather(w[number].T, "s", axis=0) for w in weights[:2])
            return gate, up, lax.all_gather(weights[2][number], "s", axis=0, tiled=True)

        full = [fetched(number) for number in range(layers)]
        h, kept = x[0], []
        a = normed(h)
        for number in range(layers):
            kept.append((h, a))
            if number + 1 < layers:
                gate, up, wd = full[number]
                h, a = down(hidden(a, gate, up), wd, h)
        by_h = dy[0]
        xs, rights = [], []
        for number in reversed(range(layers)):
            gate, up, wd = full[number]
            h, a = kept[number]
            xs.append(inner(a, by_h, gate, up, wd))
            rights.append((by_h, a))
            if number:
                by_h = below(xs[-1], gate, up, h, by_h)
        g = summed(xs, rights)
        g = g.reshape(layers, 3, -1, ROWS, g.shape[-1])[::-1]
        quarter = g.shape[2] * ROWS
        by_down = g[:, 0].reshape(layers, quarter, -1)

        def turned(g):
            g = g.reshape(layers, -1, ROWS, 4, g.shape[-1] // 4)
            return g.transpose(0, 4, 3, 1, 2).reshape(layers, g.shape[-1], 4 * quarter)

        gradients = [turned(g[:, 1]), turned(g[:, 2]), by_down]
        new = [adamw(w.astype(F32), m, v, g.astype(F32)) for w, m, v, g in zip(weights, m, v, gradients, strict=True)]
        return tuple(one[which] for which in range(3) for one in new)

    states, cut = P(("rep", "r", "s"), None, None), P(None, "s", None)
    return jax.shard_map(
        step,
        mesh=mesh,
        in_specs=(states, states) + (cut,) * 9,
        out_specs=(P("rep", "s", None),) * 9,
        check_vma=False,
    )
```

```python
import functools

import jax
import jax.numpy as jnp
from jax import lax
from jax.experimental import pallas as pl
from jax.experimental.pallas import tpu as pltpu
from jax.sharding import PartitionSpec as P

NAMES = ("w_gate", "w_up", "w_down")
BF, F32 = jnp.bfloat16, jnp.float32
MESH = pl.DeviceIdType.MESH
NN, TB, TA = ((((1,), (0,)), ((), ())), (((1,), (1,)), ((), ())), (((0,), (0,)), ((), ())))
VMEM = 60 * 2**20


def dot(a, b, dims):
    return lax.dot_general(a, b, dims, preferred_element_type=F32)


def whole(w):
    return jnp.concatenate([w[s] for s in range(4)], axis=1)


def scale_of(wide):
    return lax.rsqrt(jnp.mean(wide * wide, -1, keepdims=True) + 1e-6)


def normed(h):
    wide = h.astype(F32)
    return (wide * scale_of(wide)).astype(BF)


def adamw(w, m, v, g):
    m = 0.9 * m + 0.1 * g
    v = 0.95 * v + 0.05 * g * g
    step = m * lax.rsqrt(v + 1e-8) + 0.1 * w
    return (w - 0.02 * step).astype(BF), m, v


def params(axes, **more):
    return pltpu.CompilerParams(dimension_semantics=("arbitrary",) * axes, vmem_limit_bytes=VMEM, **more)


def cost(flops, bytes_):
    return pl.CostEstimate(flops=flops, bytes_accessed=bytes_, transcendentals=0)


def started(x, w_gate, w_up, w_down, tm=512, tn=1408):
    tokens, d = x.shape
    layers, wide, n = w_gate.shape
    quarter = n // 4
    steps_m = tokens // tm
    last = (n // tn) * steps_m

    def kernel(x_ref, g_ref, u_ref, d_ref, p_ref, a_ref, fg, fu, fd, a, g0, u0, turned, flat, dv, sems, local):
        t = pl.program_id(0) * steps_m + pl.program_id(1)
        s, r = lax.axis_index("s"), lax.axis_index("r")
        core, px, py, pz = s % 2, s // 2, r // 2, r % 2
        sx = s + 2 - 4 * px
        to_core, to_x = {"s": s + 1 - 2 * core}, {"s": sx}
        to_y, to_z = {"r": r + 2 - 4 * py}, {"r": r + 1 - 2 * pz}

        def item(number, own, full, base, size, by):
            def copy(kind, src, dst, to):
                return pltpu.make_async_remote_copy(
                    src_ref=src, dst_ref=dst, send_sem=sems.at[0, number, kind], recv_sem=sems.at[1, number, kind],
                    device_id=to, device_id_type=MESH,
                )

            def relay(kind, rows, to):
                return copy(kind, full(sx, rows), full(sx, rows), to)

            every = pl.ds(base, size)
            if by in ("y", "z"):
                half = size // 2
                par = py if by == "y" else pz
                mine, theirs = pl.ds(base + par * half, half), pl.ds(base + (1 - par) * half, half)
                out = {
                    "x": copy(0, own(mine), full(s, mine), to_x),
                    "r": relay(2, mine, to_y if by == "y" else to_z),
                    "cx": relay(3, mine, to_core),
                    "cr": relay(4, theirs, to_core),
                }
            else:
                part = size // 4

                def at(y, z):
                    return pl.ds(base + (2 * y + z) * part, part)

                mine = at(py, pz)
                out = {
                    "x": copy(0, own(mine), full(s, mine), to_x),
                    "y": relay(2, mine, to_y),
                    "z": relay(3, mine, to_z),
                    "cx": relay(4, mine, to_core),
                    "cy": relay(5, at(1 - py, pz), to_core),
                    "cz": relay(6, at(py, 1 - pz), to_core),
                    "d": relay(7, at(1 - py, pz), to_z) if by == "yz" else relay(7, at(py, 1 - pz), to_y),
                    "cd": relay(8, at(1 - py, 1 - pz), to_core),
                }
            out["c"] = copy(1, own(every), full(s, every), to_core)
            return out

        def inside(ref):
            return (lambda rows: ref.at[s, rows]), (lambda block, rows: ref.at[block, rows])

        def outside(own, ref):
            return (lambda rows: own.at[rows]), (lambda block, rows: ref.at[1, block, rows])

        g0a, u0a = item(0, *inside(g0), 0, tn, "y"), item(1, *inside(u0), 0, tn, "z")
        g0b, u0b = item(2, *inside(g0), tn, tn, "y"), item(3, *inside(u0), tn, tn, "z")
        d0 = item(4, lambda rows: d_ref.at[0, rows], lambda block, rows: fd.at[0, block, rows], 0, quarter, "yz")
        g1 = item(5, *outside(turned.at[0], fg), 0, n, "zy")
        u1 = item(6, *outside(turned.at[1], fu), 0, n, "yz")
        d1 = item(7, lambda rows: d_ref.at[1, rows], lambda block, rows: fd.at[1, block, rows], 0, quarter, "zy")
        items = (g0a, u0a, g0b, u0b, d0, g1, u1, d1)

        def here(k, src, dst):
            return pltpu.make_async_copy(src, dst, local.at[k])

        loads = [here(2 * i + j, ref.at[i], flat.at[2 * i + j]) for i in range(2) for j, ref in enumerate((g_ref, u_ref))]
        load_x, load_d = here(4, x_ref, a), here(5, d_ref, dv)
        keep = [
            here(6, turned.at[0], fg.at[1, s]),
            here(7, turned.at[1], fu.at[1, s]),
            here(8, dv.at[0], fd.at[0, s]),
            here(9, dv.at[1], fd.at[1, s]),
            here(10, a, a_ref),
            here(11, g0, fg.at[0]),
            here(12, u0, fu.at[0]),
        ]

        def begin(one):
            one["x"].start()
            one["c"].start()

        def got(one, *kinds):
            for kind in kinds:
                one[kind].wait_recv()

        def go(one, *kinds):
            for kind in kinds:
                one[kind].start()

        @pl.when(t == 0)
        def _():
            for load in (*loads[:2], load_x, load_d, *loads[2:]):
                load.start()
            barrier = pltpu.get_barrier_semaphore()
            for to in (to_core, to_x, to_y, to_z):
                pl.semaphore_signal(barrier, inc=1, device_id=to, device_id_type=MESH)
            pl.semaphore_wait(barrier, 4)
            loads[0].wait()
            loads[1].wait()
            for base, pair in ((0, (g0a, u0a)), (tn, (g0b, u0b))):
                for j, (ref, one) in enumerate(zip((g0, u0), pair, strict=True)):
                    ref[s, base : base + tn] = flat[j, :, base : base + tn].T
                    begin(one)
            begin(d0)
            load_x.wait()

            @pl.loop(0, steps_m)
            def _(i):
                rows = pl.ds(i * tm, tm)
                a[rows, :] = normed(a[rows, :])

            keep[4].start()
            got(g0a, "x")
            go(g0a, "r", "cx")
            for j, one in enumerate((g1, u1)):
                loads[2 + j].wait()
                for base in (0, tn):
                    turned[j, base : base + tn] = flat[2 + j, :, base : base + tn].T
                begin(one)
                keep[j].start()
            begin(d1)
            load_d.wait()
            keep[2].start()
            keep[3].start()
            got(u0a, "x")
            go(u0a, "r", "cx")
            got(g0a, "r")
            go(g0a, "cr")
            got(u0a, "r")
            go(u0a, "cr")
            got(g0a, "c", "cx", "cr")
            got(u0a, "c", "cx", "cr")

        def on(step, *todo):
            @pl.when(t == step)
            def _():
                for one, wait, then in todo:
                    got(one, *wait)
                    go(one, *then)

        on(1, (g0b, ("x",), ("r", "cx")))
        on(3, (u0b, ("x",), ("r", "cx")))
        on(4, (g0b, ("r",), ("cr",)))
        on(5, (d0, ("x",), ("y", "z", "cx")))
        on(6, (u0b, ("r",), ("cr",)))
        on(7, (g1, ("x",), ("y", "z", "cx")))

        @pl.when(t == steps_m)
        def _():
            got(g0b, "c", "cx", "cr")
            got(u0b, "c", "cx", "cr")
            keep[5].start()
            keep[6].start()

        on(8, (d0, ("y", "z"), ("cy", "cz", "d")))
        on(9, (u1, ("x",), ("y", "z", "cx")))
        on(10, (g1, ("y", "z"), ("cy", "cz", "d")))
        on(11, (d1, ("x",), ("y", "z", "cx")), (d0, ("d",), ("cd",)))
        on(12, (u1, ("y", "z"), ("cy", "cz", "d")))
        on(13, (g1, ("d",), ("cd",)))
        on(14, (d1, ("y", "z"), ("cy", "cz", "d")))
        on(15, (u1, ("d",), ("cd",)))

        rows = pl.ds(pl.program_id(1) * tm, tm)
        columns = pl.ds(pl.program_id(0) * tn, tn)
        block = a[rows, :]
        gate = dot(block, whole([g0[q, columns] for q in range(4)]), TB)
        up = dot(block, whole([u0[q, columns] for q in range(4)]), TB)
        p_ref[...] = (gate * jax.nn.sigmoid(gate) * up).astype(BF)

        @pl.when(t == last - 1)
        def _():
            got(d1, "d")
            go(d1, "cd")
            for one in (d0, g1, u1, d1):
                got(one, "c", "cx", "cy", "cz", "cd")
            for one in items:
                for copy in one.values():
                    copy.wait_send()
            for copy in keep:
                copy.wait()

    hbm = pl.BlockSpec(memory_space=pl.ANY)
    dma = pltpu.SemaphoreType.DMA
    full = jax.ShapeDtypeStruct((layers, 4, n, wide), BF)
    return pl.pallas_call(
        kernel,
        out_shape=(
            jax.ShapeDtypeStruct((tokens, n), BF),
            jax.ShapeDtypeStruct((tokens, d), BF),
            full,
            full,
            jax.ShapeDtypeStruct((layers, 4, quarter, d), BF),
        ),
        grid=(n // tn, steps_m),
        in_specs=[hbm] * 4,
        out_specs=(pl.BlockSpec((tm, tn), lambda n, m: (m, n)), hbm, hbm, hbm, hbm),
        scratch_shapes=[
            pltpu.VMEM((tokens, d), BF),
            pltpu.VMEM((4, n, wide), BF),
            pltpu.VMEM((4, n, wide), BF),
            pltpu.VMEM((2, n, wide), BF),
            pltpu.VMEM((4, wide, n), BF),
            pltpu.VMEM((layers, quarter, d), BF),
            dma((2, 8, 9)),
            dma((13,)),
        ],
        compiler_params=params(2, collective_id=1, has_side_effects=True),
        cost_estimate=cost(4 * tokens * d * n, 2 * tokens * (d + n)),
        name="started",
    )(x, w_gate, w_up, w_down)


def down(p, wd, layer, h, tm=512):
    tokens, n = p.shape
    d = h.shape[1]

    def kernel(p, w, h, ho, ao):
        new = h[...] + dot(p[...], w[...], NN).astype(BF)
        ho[...] = new
        ao[...] = normed(new)

    row = pl.BlockSpec((tm, d), lambda m: (m, 0))
    return pl.pallas_call(
        kernel,
        out_shape=(jax.ShapeDtypeStruct((tokens, d), BF),) * 2,
        grid=(tokens // tm,),
        in_specs=[pl.BlockSpec((tm, n), lambda m: (m, 0)), pl.BlockSpec((None, n, d), lambda m: (layer, 0, 0)), row],
        out_specs=(row, row),
        compiler_params=params(1),
        cost_estimate=cost(2 * tokens * d * n, 2 * tokens * (3 * d + n)),
        name="down",
    )(p, wd, h)


def inner(a, dy, wg, wu, wd, layer, tm=512, tn=704):
    tokens, d = a.shape
    n = wd.shape[1]

    def kernel(a, dy, g, u, w, o):
        gate, up = dot(whole(g), a[...], TB), dot(whole(u), a[...], TB)
        by_p = dot(w[...], dy[...], TB).astype(BF).astype(F32)
        sig = jax.nn.sigmoid(gate)
        act = gate * sig
        o[0] = (act * up).astype(BF)
        o[1] = (by_p * up * (sig * (1.0 + gate * (1.0 - sig)))).astype(BF)
        o[2] = (by_p * act).astype(BF)

    w = pl.BlockSpec((None, 4, tn, d // 4), lambda n, m: (layer, 0, n, 0))
    act = pl.BlockSpec((tm, d), lambda n, m: (m, 0))
    return pl.pallas_call(
        kernel,
        out_shape=jax.ShapeDtypeStruct((3, n, tokens), BF),
        grid=(n // tn, tokens // tm),
        in_specs=[act, act, w, w, pl.BlockSpec((None, tn, d), lambda n, m: (layer, n, 0))],
        out_specs=pl.BlockSpec((3, tn, tm), lambda n, m: (0, n, m)),
        compiler_params=params(2),
        cost_estimate=cost(6 * tokens * d * n, 2 * tokens * (2 * d + 3 * n)),
        name="inner",
    )(a, dy, wg, wu, wd)


def below(x, wg, wu, layer, h, dh, tm=256):
    tokens, d = h.shape
    n = x.shape[1]

    def kernel(x, g, u, h, dh, o):
        by_a = dot(x[0], whole(g), TA).astype(BF).astype(F32) + dot(x[1], whole(u), TA).astype(BF).astype(F32)
        wide = h[...].astype(F32)
        r = scale_of(wide)
        by_h = by_a * r - wide * (r * r * r) * jnp.mean(by_a * wide, -1, keepdims=True)
        o[...] = dh[...] + by_h.astype(BF)

    row = pl.BlockSpec((tm, d), lambda m: (m, 0))
    w = pl.BlockSpec((None, 4, n, d // 4), lambda m: (layer, 0, 0, 0))

    def two(x_gate, x_up, g, u, h, dh, o):
        kernel((x_gate[0], x_up[0]), g, u, h, dh, o)

    return pl.pallas_call(
        two,
        out_shape=jax.ShapeDtypeStruct((tokens, d), BF),
        grid=(tokens // tm,),
        in_specs=[pl.BlockSpec((1, n, tm), lambda m: (1, 0, m)), pl.BlockSpec((1, n, tm), lambda m: (2, 0, m)), w, w, row, row],
        out_specs=row,
        compiler_params=params(1),
        cost_estimate=cost(4 * tokens * d * n, 2 * tokens * (3 * d + 2 * n)),
        name="below",
    )(x, x, wg, wu, h, dh)


LAG = (0, 1, 3, 5, 7)
ROWS = 64


def summed(xs, rights):
    _, n, tokens = xs[0].shape
    d = rights[0][0].shape[1]
    quarter = n // 4
    per = quarter // ROWS
    layers = len(xs)
    chunks = layers * 3 * per
    wide = d // 4
    slots = 4

    def kernel(*refs):
        x_refs, r_refs = refs[: 2 * layers], refs[2 * layers : 4 * layers]
        out, right, acc, csend, crecv, mine, xsend, xrecv, ysend, yrecv, zsend, zrecv, rsem, csems, xsems, ysems, zsems = refs[4 * layers :]
        t = pl.program_id(0)
        s, r = lax.axis_index("s"), lax.axis_index("r")
        core, x, y, z = s % 2, s // 2, r // 2, r % 2
        other, over_x, over_y, over_z = s + 1 - 2 * core, s + 2 - 4 * x, r + 2 - 4 * y, r + 1 - 2 * z

        def load(i):
            return pltpu.make_async_copy(r_refs[i], right.at[i % 2], rsem.at[i % 2])

        def send(src, dst, sems, slot, to):
            return pltpu.make_async_remote_copy(
                src_ref=src.at[slot], dst_ref=dst.at[slot], send_sem=sems.at[0, slot], recv_sem=sems.at[1, slot],
                device_id=to, device_id_type=MESH,
            )

        def along_core(u):
            return send(csend, crecv, csems, u % 2, {"s": other})

        def along_x(u):
            return send(xsend, xrecv, xsems, u % slots, {"s": over_x})

        def along_y(u):
            return send(ysend, yrecv, ysems, u % slots, {"r": over_y})

        def along_z(u):
            return send(zsend, zrecv, zsems, u % slots, {"r": over_z})

        @pl.when(t == 0)
        def _():
            load(0).start()
            load(1).start()
            barrier = pltpu.get_barrier_semaphore()
            for to in ({"s": other}, {"s": over_x}, {"r": over_y}, {"r": over_z}):
                pl.semaphore_signal(barrier, inc=1, device_id=to, device_id_type=MESH)
            pl.semaphore_wait(barrier, 4)

        for layer in range(layers):
            first = layer * 3 * per

            @pl.when(t == first)
            def _():
                load(2 * layer).wait()
                if layer:
                    load(2 * layer + 1).start()

            @pl.when(t == first + per)
            def _():
                load(2 * layer + 1).wait()
                if layer + 1 < layers:
                    load(2 * layer + 2).start()

            @pl.when((t >= first) & (t < first + per))
            def _():
                o = dot(x_refs[2 * layer][...].reshape(4 * ROWS, tokens), right[0], NN)
                for q in range(4):
                    acc[t % 2, q] = o[ROWS * q : ROWS * (q + 1)]

            @pl.when((t >= first + per) & (t < first + 3 * per))
            def _():
                o = dot(x_refs[2 * layer + 1][...], right[1], NN)
                for q in range(4):
                    for p in range(4):
                        acc[t % 2, p, :, wide * q : wide * (q + 1)] = o[ROWS * q : ROWS * (q + 1), wide * p : wide * (p + 1)]

        @pl.when(t >= LAG[4])
        def _():
            u = t - LAG[4]
            along_z(u).wait()
            out[0] = (zsend[u % slots].astype(F32) + zrecv[u % slots].astype(F32)).astype(BF)

        @pl.when((t >= LAG[3]) & (t < chunks + LAG[3]))
        def _():
            u = t - LAG[3]
            along_y(u).wait()
            zsend[u % slots] = (ysend[u % slots].astype(F32) + yrecv[u % slots].astype(F32)).astype(BF)
            along_z(u).start()

        @pl.when((t >= LAG[2]) & (t < chunks + LAG[2]))
        def _():
            u = t - LAG[2]
            along_x(u).wait()
            ysend[u % slots] = (mine[u % slots] + xrecv[u % slots].astype(F32)).astype(BF)
            along_y(u).start()

        @pl.when((t >= LAG[1]) & (t < chunks + LAG[1]))
        def _():
            u = t - LAG[1]
            along_core(u).wait()
            xsend[u % slots] = (acc[u % 2, 2 - 2 * x + core] + crecv[u % 2, 1 - x].astype(F32)).astype(BF)
            along_x(u).start()
            mine[u % slots] = acc[u % 2, 2 * x + core] + crecv[u % 2, x].astype(F32)

        @pl.when(t < chunks)
        def _():
            for j in range(2):
                csend[t % 2, j] = acc[t % 2, 2 * j + 1 - core].astype(BF)
            along_core(t).start()

    def lhs(layer):
        def pieces(t):
            return 0, 0, jnp.clip(t - layer * 3 * per, 0, per - 1), 0

        def rows(t):
            u = jnp.clip(t - layer * 3 * per - per, 0, 2 * per - 1)
            return 1 + u // per, u % per, 0

        return [pl.BlockSpec((None, 4, ROWS, tokens), pieces), pl.BlockSpec((None, 4 * ROWS, tokens), rows)]

    block = (ROWS, d)
    dma = pltpu.SemaphoreType.DMA
    return pl.pallas_call(
        kernel,
        out_shape=jax.ShapeDtypeStruct((chunks,) + block, BF),
        grid=(chunks + LAG[4],),
        in_specs=[spec for layer in range(layers) for spec in lhs(layer)] + [pl.BlockSpec(memory_space=pl.ANY)] * (2 * layers),
        out_specs=pl.BlockSpec((1,) + block, lambda t: (jnp.maximum(t - LAG[4], 0), 0, 0)),
        scratch_shapes=[
            pltpu.VMEM((2, tokens, d), BF),
            pltpu.VMEM((2, 4) + block, F32),
            pltpu.VMEM((2, 2) + block, BF),
            pltpu.VMEM((2, 2) + block, BF),
            pltpu.VMEM((slots,) + block, F32),
        ]
        + [pltpu.VMEM((slots,) + block, BF)] * 6
        + [dma((2,)), dma((2, 2)), dma((2, slots)), dma((2, slots)), dma((2, slots))],
        compiler_params=params(1, collective_id=0, has_side_effects=True),
        cost_estimate=cost(2 * chunks * 4 * ROWS * tokens * d, 2 * layers * tokens * (3 * n + 2 * d)),
        name="summed",
    )(*[view for x in xs for view in (x.reshape(3, 4, quarter, tokens), x)], *[r for pair in rights for r in pair])


def stepped(g, weights, ms, vs):
    layers, quarter, d = weights[2].shape
    per = quarter // ROWS
    wide = d // 4

    def kernel(*refs):
        for j in range(3):
            g = refs[j][...].astype(F32)
            if j < 2:
                g = jnp.concatenate([g[:, wide * q : wide * (q + 1)] for q in range(4)], axis=0).T
            new = adamw(refs[3 + j][...].astype(F32), refs[6 + j][...], refs[9 + j][...], g)
            for which in range(3):
                refs[12 + 3 * which + j][...] = new[which]

    def chunk(j):
        return pl.BlockSpec((None, ROWS, d), lambda l, k: ((layers - 1 - l) * 3 * per + j * per + k, 0, 0))

    column = pl.BlockSpec((None, wide, 4 * ROWS), lambda l, k: (l, 0, k))
    blocks = [column, column, pl.BlockSpec((None, ROWS, d), lambda l, k: (l, k, 0))]
    return pl.pallas_call(
        kernel,
        out_shape=tuple(jax.ShapeDtypeStruct(a.shape, a.dtype) for a in (*weights, *ms, *vs)),
        grid=(layers, per),
        in_specs=[chunk(1), chunk(2), chunk(0)] + blocks * 3,
        out_specs=tuple(blocks * 3),
        compiler_params=params(2),
        cost_estimate=cost(20 * layers * 3 * quarter * d, 22 * layers * 3 * quarter * d),
        name="stepped",
    )(g, g, g, *weights, *ms, *vs)


def solution(mesh):
    def step(x, dy, *arrays):
        weights, m, v = (arrays[i : i + 3] for i in (0, 3, 6))
        layers, quarter, d = weights[2].shape
        h = x[0]
        p, a, gate, up, wd = started(h, *weights)
        wd = wd.reshape(layers, 4 * quarter, d)
        kept = [(h, a)]
        h, a = down(p, wd, 0, h)
        kept.append((h, a))
        by_h = dy[0]
        xs, rights = [], []
        for number in reversed(range(layers)):
            h, a = kept[number]
            xs.append(inner(a, by_h, gate, up, wd, number))
            rights.append((by_h, a))
            if number:
                by_h = below(xs[-1], gate, up, number, h, by_h)
        return stepped(summed(xs, rights), weights, m, v)

    states, cut = P(("rep", "r", "s"), None, None), P(None, "s", None)
    return jax.shard_map(
        step,
        mesh=mesh,
        in_specs=(states, states) + (cut,) * 9,
        out_specs=(P("rep", "s", None),) * 9,
        check_vma=False,
    )
```

```python
import functools

import jax
import jax.numpy as jnp
from jax import lax
from jax.experimental import pallas as pl
from jax.experimental.pallas import tpu as pltpu
from jax.sharding import PartitionSpec as P

NAMES = ("w_gate", "w_up", "w_down")
BF, F32 = jnp.bfloat16, jnp.float32
MESH = pl.DeviceIdType.MESH
NN, TB, TA = ((((1,), (0,)), ((), ())), (((1,), (1,)), ((), ())), (((0,), (0,)), ((), ())))
VMEM = 60 * 2**20


def dot(a, b, dims):
    return lax.dot_general(a, b, dims, preferred_element_type=F32)


def whole(w):
    return jnp.concatenate([w[s] for s in range(4)], axis=1)


def scale_of(wide):
    return lax.rsqrt(jnp.mean(wide * wide, -1, keepdims=True) + 1e-6)


def normed(h):
    wide = h.astype(F32)
    return (wide * scale_of(wide)).astype(BF)


def adamw(w, m, v, g):
    m = 0.9 * m + 0.1 * g
    v = 0.95 * v + 0.05 * g * g
    step = m * lax.rsqrt(v + 1e-8) + 0.1 * w
    return (w - 0.02 * step).astype(BF), m, v


def params(axes, **more):
    return pltpu.CompilerParams(dimension_semantics=("arbitrary",) * axes, vmem_limit_bytes=VMEM, **more)


def cost(flops, bytes_):
    return pl.CostEstimate(flops=flops, bytes_accessed=bytes_, transcendentals=0)


def routes(sems):
    s, r = lax.axis_index("s"), lax.axis_index("r")
    core, px, py, pz = s % 2, s // 2, r // 2, r % 2
    sx = s + 2 - 4 * px
    to_core, to_x = {"s": s + 1 - 2 * core}, {"s": sx}
    to_y, to_z = {"r": r + 2 - 4 * py}, {"r": r + 1 - 2 * pz}

    def item(number, own, full, base, size, by):
        def copy(kind, src, dst, to):
            return pltpu.make_async_remote_copy(
                src_ref=src, dst_ref=dst, send_sem=sems.at[0, number, kind], recv_sem=sems.at[1, number, kind],
                device_id=to, device_id_type=MESH,
            )

        def relay(kind, rows, to):
            return copy(kind, full(sx, rows), full(sx, rows), to)

        every = pl.ds(base, size)
        if by in ("y", "z"):
            half = size // 2
            par = py if by == "y" else pz
            mine, theirs = pl.ds(base + par * half, half), pl.ds(base + (1 - par) * half, half)
            out = {
                "x": copy(0, own(mine), full(s, mine), to_x),
                "r": relay(2, mine, to_y if by == "y" else to_z),
                "cx": relay(3, mine, to_core),
                "cr": relay(4, theirs, to_core),
            }
        else:
            part = size // 4

            def at(y, z):
                return pl.ds(base + (2 * y + z) * part, part)

            mine = at(py, pz)
            out = {
                "x": copy(0, own(mine), full(s, mine), to_x),
                "y": relay(2, mine, to_y),
                "z": relay(3, mine, to_z),
                "cx": relay(4, mine, to_core),
                "cy": relay(5, at(1 - py, pz), to_core),
                "cz": relay(6, at(py, 1 - pz), to_core),
                "d": relay(7, at(1 - py, pz), to_z) if by == "yz" else relay(7, at(py, 1 - pz), to_y),
                "cd": relay(8, at(1 - py, 1 - pz), to_core),
            }
        out["c"] = copy(1, own(every), full(s, every), to_core)
        return out

    return item, s, (to_core, to_x, to_y, to_z)


def greet(partners):
    barrier = pltpu.get_barrier_semaphore()
    for to in partners:
        pl.semaphore_signal(barrier, inc=1, device_id=to, device_id_type=MESH)
    pl.semaphore_wait(barrier, len(partners))


def got(one, *kinds):
    for kind in kinds:
        one[kind].wait_recv()


def go(one, *kinds):
    for kind in kinds:
        one[kind].start()


FOUR = ("c", "cx", "cy", "cz", "cd")
TILES = (512, 896, 1408)


def started(x, w_gate, w_up, w_down, tm=512):
    tokens, d = x.shape
    layers, wide, n = w_gate.shape
    quarter = n // 4
    steps_m = tokens // tm
    bases = tuple(sum(TILES[:i]) for i in range(len(TILES)))
    last = len(TILES) * steps_m

    def kernel(x_ref, g_ref, u_ref, d_ref, p0, p1, p2, a_ref, fg, fu, fd, a, g0, u0, turned, flat, dv, sems, local):
        t = pl.program_id(0)
        item, s, partners = routes(sems)

        def inside(ref):
            return (lambda rows: ref.at[s, rows]), (lambda block, rows: ref.at[block, rows])

        def outside(own, ref):
            return (lambda rows: own.at[rows]), (lambda block, rows: ref.at[1, block, rows])

        tiles = [
            (item(2 * i, *inside(g0), bases[i], TILES[i], "y"), item(2 * i + 1, *inside(u0), bases[i], TILES[i], "z"))
            for i in range(len(TILES))
        ]
        d0 = item(6, lambda rows: d_ref.at[0, rows], lambda block, rows: fd.at[block, rows], 0, quarter, "yz")
        half = n // 2
        g1a, u1a = item(7, *outside(turned.at[0], fg), 0, half, "zy"), item(8, *outside(turned.at[1], fu), 0, half, "yz")
        g1b, u1b = item(9, *outside(turned.at[0], fg), half, half, "zy"), item(10, *outside(turned.at[1], fu), half, half, "yz")
        late = (d0, g1a, u1a, g1b, u1b)

        def here(k, src, dst):
            return pltpu.make_async_copy(src, dst, local.at[k])

        loads = [here(2 * i + j, ref.at[i], flat.at[2 * i + j]) for i in range(2) for j, ref in enumerate((g_ref, u_ref))]
        load_x, load_d = here(4, x_ref, a), here(5, d_ref.at[0], dv)
        keep = [
            here(6, turned.at[0], fg.at[1, s]),
            here(7, turned.at[1], fu.at[1, s]),
            here(8, dv, fd.at[s]),
            here(9, a, a_ref),
            here(10, g0, fg.at[0]),
            here(11, u0, fu.at[0]),
        ]

        @pl.when(t == 0)
        def _():
            for load in (*loads[:2], load_x, load_d, *loads[2:]):
                load.start()
            greet(partners)
            loads[0].wait()
            loads[1].wait()
            for base, size, pair in zip(bases, TILES, tiles, strict=True):
                for j, (ref, one) in enumerate(zip((g0, u0), pair, strict=True)):
                    ref[s, base : base + size] = flat[j, :, base : base + size].T
                    go(one, "x", "c")
            go(d0, "x", "c")
            load_x.wait()

            @pl.loop(0, steps_m)
            def _(i):
                rows = pl.ds(i * tm, tm)
                a[rows, :] = normed(a[rows, :])

            keep[3].start()
            g00, u00 = tiles[0]
            got(g00, "x")
            go(g00, "r", "cx")
            got(u00, "x")
            go(u00, "r", "cx")
            got(g00, "r")
            go(g00, "cr")
            got(u00, "r")
            go(u00, "cr")
            for j in range(2):
                loads[2 + j].wait()
                for base in (0, half):
                    turned[j, base : base + half] = flat[2 + j, :, base : base + half].T
                keep[j].start()
            for one in late[1:]:
                go(one, "x", "c")
            load_d.wait()
            keep[2].start()

        def on(step, *todo):
            @pl.when(t == step)
            def _():
                for one, wait, then in todo:
                    got(one, *wait)
                    go(one, *then)

        (_, _), (g01, u01), (g02, u02) = tiles
        first, second, third = (("x",), ("y", "z", "cx")), (("y", "z"), ("cy", "cz", "d")), (("d",), ("cd",))
        near, far = (("x",), ("r", "cx")), (("r",), ("cr",))
        on(1, (g01, *near))
        on(3, (u01, *near))
        on(6, (g01, *far))
        on(8, (u01, *far), (g02, *near))
        on(11, (u02, *near))
        on(12, (g02, *far))
        on(14, (d0, *first))
        on(16, (u02, *far), (g1a, *first))
        on(17, (u1a, *first))
        on(18, (d0, *second), (g1b, *first))
        on(19, (g1a, *second), (u1b, *first))
        on(20, (u1a, *second))
        on(21, (g1b, *second), (d0, *third))
        on(22, (u1b, *second), (g1a, *third))
        on(23, (u1a, *third))

        for i, (base, size, pair, p_ref) in enumerate(zip(bases, TILES, tiles, (p0, p1, p2), strict=True)):

            @pl.when(t == i * steps_m)
            def _():
                for one in pair:
                    got(one, "c", "cx", "cr")
                if i == len(TILES) - 1:
                    keep[4].start()
                    keep[5].start()

            @pl.when((t >= i * steps_m) & (t < (i + 1) * steps_m))
            def _():
                block = a[pl.ds((t - i * steps_m) * tm, tm), :]
                gate = dot(block, whole([g0[q, base : base + size] for q in range(4)]), TB)
                up = dot(block, whole([u0[q, base : base + size] for q in range(4)]), TB)
                p_ref[...] = (gate * jax.nn.sigmoid(gate) * up).astype(BF)

        @pl.when(t == last - 1)
        def _():
            for one in (g1b, u1b):
                got(one, "d")
                go(one, "cd")
            for one in late:
                got(one, *FOUR)
            for one in (*[one for pair in tiles for one in pair], *late):
                for copy in one.values():
                    copy.wait_send()
            for copy in keep:
                copy.wait()

    def part(i):
        return pl.BlockSpec((tm, TILES[i]), lambda t: (jnp.clip(t - i * steps_m, 0, steps_m - 1), 0))

    hbm = pl.BlockSpec(memory_space=pl.ANY)
    dma = pltpu.SemaphoreType.DMA
    full = jax.ShapeDtypeStruct((layers, 4, n, wide), BF)
    return pl.pallas_call(
        kernel,
        out_shape=(
            *[jax.ShapeDtypeStruct((tokens, size), BF) for size in TILES],
            jax.ShapeDtypeStruct((tokens, d), BF),
            full,
            full,
            jax.ShapeDtypeStruct((4, quarter, d), BF),
        ),
        grid=(last,),
        in_specs=[hbm] * 4,
        out_specs=(*[part(i) for i in range(len(TILES))], hbm, hbm, hbm, hbm),
        scratch_shapes=[
            pltpu.VMEM((tokens, d), BF),
            pltpu.VMEM((4, n, wide), BF),
            pltpu.VMEM((4, n, wide), BF),
            pltpu.VMEM((2, n, wide), BF),
            pltpu.VMEM((4, wide, n), BF),
            pltpu.VMEM((quarter, d), BF),
            dma((2, 11, 9)),
            dma((12,)),
        ],
        compiler_params=params(1, collective_id=1, has_side_effects=True),
        cost_estimate=cost(4 * tokens * d * n, 2 * tokens * (d + n)),
        name="started",
    )(x, w_gate, w_up, w_down)


def down(ps, wd, h, w_down, tm=512):
    tokens, d = h.shape
    n = wd.shape[0]
    quarter = n // 4
    steps = tokens // tm
    bases = tuple(sum(TILES[:i]) for i in range(len(TILES)))
    cut = 384

    def kernel(p0, p1, p2, w, h, d_ref, ho, ao, fd, dv, sems, local):
        t = pl.program_id(0)
        item, s, partners = routes(sems)

        def one(number, base, size, by):
            return item(number, lambda rows: d_ref.at[1, rows], lambda block, rows: fd.at[block, rows], base, size, by)

        a, b = one(0, 0, cut, "yz"), one(1, cut, quarter - cut, "zy")
        load = pltpu.make_async_copy(d_ref.at[1], dv, local.at[0])
        keep = pltpu.make_async_copy(dv, fd.at[s], local.at[1])

        @pl.when(t == 0)
        def _():
            load.start()
            greet(partners)
            for which in (a, b):
                go(which, "x", "c")
            load.wait()
            keep.start()

        for step, which, wait, then in (
            (2, a, ("x",), ("y", "z", "cx")),
            (3, b, ("x",), ("y", "z", "cx")),
            (4, a, ("y", "z"), ("cy", "cz", "d")),
            (5, b, ("y", "z"), ("cy", "cz", "d")),
            (6, a, ("d",), ("cd",)),
            (7, b, ("d",), ("cd",)),
        ):

            @pl.when(t == step)
            def _():
                got(which, *wait)
                go(which, *then)

        by_p = sum(dot(p[...], w[base : base + size], NN) for p, base, size in zip((p0, p1, p2), bases, TILES, strict=True))
        new = h[...] + by_p.astype(BF)
        ho[...] = new
        ao[...] = normed(new)

        @pl.when(t == steps - 1)
        def _():
            for which in (a, b):
                got(which, *FOUR)
                for copy in which.values():
                    copy.wait_send()
            keep.wait()

    row = pl.BlockSpec((tm, d), lambda m: (m, 0))
    hbm = pl.BlockSpec(memory_space=pl.ANY)
    dma = pltpu.SemaphoreType.DMA
    return pl.pallas_call(
        kernel,
        out_shape=(*[jax.ShapeDtypeStruct((tokens, d), BF)] * 2, jax.ShapeDtypeStruct((4, quarter, d), BF)),
        grid=(steps,),
        in_specs=[pl.BlockSpec((tm, size), lambda m: (m, 0)) for size in TILES] + [pl.BlockSpec((n, d), lambda m: (0, 0)), row, hbm],
        out_specs=(row, row, hbm),
        scratch_shapes=[pltpu.VMEM((quarter, d), BF), dma((2, 2, 9)), dma((2,))],
        compiler_params=params(1, collective_id=2, has_side_effects=True),
        cost_estimate=cost(2 * tokens * d * n, 2 * tokens * (3 * d + n)),
        name="down",
    )(*ps, wd, h, w_down)


def inner(a, dy, wg, wu, wd, layer, tm=1024, tn=704, lanes=256):
    tokens, d = a.shape
    n = wd.shape[0]

    def kernel(a, dy, g, u, w, o):
        to_gate, to_up = whole(g), whole(u)
        for start in range(0, tm, lanes):
            part = slice(start, start + lanes)
            gate, up = dot(to_gate, a[part], TB), dot(to_up, a[part], TB)
            by_p = dot(w[...], dy[part], TB).astype(BF).astype(F32)
            sig = 0.5 * jnp.tanh(0.5 * gate) + 0.5
            act = gate * sig
            o[0, :, part] = (act * up).astype(BF)
            o[1, :, part] = (by_p * up * (sig * (1.0 + gate * (1.0 - sig)))).astype(BF)
            o[2, :, part] = (by_p * act).astype(BF)

    w = pl.BlockSpec((None, 4, tn, d // 4), lambda n, m: (layer, 0, n, 0))
    act = pl.BlockSpec((tm, d), lambda n, m: (m, 0))
    return pl.pallas_call(
        kernel,
        out_shape=jax.ShapeDtypeStruct((3, n, tokens), BF),
        grid=(n // tn, tokens // tm),
        in_specs=[act, act, w, w, pl.BlockSpec((tn, d), lambda n, m: (n, 0))],
        out_specs=pl.BlockSpec((3, tn, tm), lambda n, m: (0, n, m)),
        compiler_params=params(2),
        cost_estimate=cost(6 * tokens * d * n, 2 * tokens * (2 * d + 3 * n)),
        name="inner",
    )(a, dy, wg, wu, wd)


def below(x, wg, wu, layer, h, dh, tm=256):
    tokens, d = h.shape
    n = x.shape[1]

    def kernel(x, g, u, h, dh, o):
        by_a = dot(x[0], whole(g), TA).astype(BF).astype(F32) + dot(x[1], whole(u), TA).astype(BF).astype(F32)
        wide = h[...].astype(F32)
        r = scale_of(wide)
        by_h = by_a * r - wide * (r * r * r) * jnp.mean(by_a * wide, -1, keepdims=True)
        o[...] = dh[...] + by_h.astype(BF)

    row = pl.BlockSpec((tm, d), lambda m: (m, 0))
    w = pl.BlockSpec((None, 4, n, d // 4), lambda m: (layer, 0, 0, 0))

    def two(x_gate, x_up, g, u, h, dh, o):
        kernel((x_gate[0], x_up[0]), g, u, h, dh, o)

    return pl.pallas_call(
        two,
        out_shape=jax.ShapeDtypeStruct((tokens, d), BF),
        grid=(tokens // tm,),
        in_specs=[pl.BlockSpec((1, n, tm), lambda m: (1, 0, m)), pl.BlockSpec((1, n, tm), lambda m: (2, 0, m)), w, w, row, row],
        out_specs=row,
        compiler_params=params(1),
        cost_estimate=cost(4 * tokens * d * n, 2 * tokens * (3 * d + 2 * n)),
        name="below",
    )(x, x, wg, wu, h, dh)


LAG = (0, 1, 3, 5, 7)
ROWS = 64


def summed(xs, rights):
    _, n, tokens = xs[0].shape
    d = rights[0][0].shape[1]
    quarter = n // 4
    per = quarter // ROWS
    layers = len(xs)
    chunks = layers * 3 * per
    wide = d // 4
    slots = 4

    def kernel(*refs):
        x_refs, r_refs = refs[: 2 * layers], refs[2 * layers : 4 * layers]
        out, right, acc, csend, crecv, mine, xsend, xrecv, ysend, yrecv, zsend, zrecv, rsem, csems, xsems, ysems, zsems = refs[4 * layers :]
        t = pl.program_id(0)
        s, r = lax.axis_index("s"), lax.axis_index("r")
        core, x, y, z = s % 2, s // 2, r // 2, r % 2
        other, over_x, over_y, over_z = s + 1 - 2 * core, s + 2 - 4 * x, r + 2 - 4 * y, r + 1 - 2 * z

        def load(i):
            return pltpu.make_async_copy(r_refs[i], right.at[i % 2], rsem.at[i % 2])

        def send(src, dst, sems, slot, to):
            return pltpu.make_async_remote_copy(
                src_ref=src.at[slot], dst_ref=dst.at[slot], send_sem=sems.at[0, slot], recv_sem=sems.at[1, slot],
                device_id=to, device_id_type=MESH,
            )

        def along_core(u):
            return send(csend, crecv, csems, u % 2, {"s": other})

        def along_x(u):
            return send(xsend, xrecv, xsems, u % slots, {"s": over_x})

        def along_y(u):
            return send(ysend, yrecv, ysems, u % slots, {"r": over_y})

        def along_z(u):
            return send(zsend, zrecv, zsems, u % slots, {"r": over_z})

        @pl.when(t == 0)
        def _():
            load(0).start()
            barrier = pltpu.get_barrier_semaphore()
            for to in ({"s": other}, {"s": over_x}, {"r": over_y}, {"r": over_z}):
                pl.semaphore_signal(barrier, inc=1, device_id=to, device_id_type=MESH)
            pl.semaphore_wait(barrier, 4)

        for layer in range(layers):
            first = layer * 3 * per

            @pl.when(t == first)
            def _():
                load(2 * layer).wait()
                load(2 * layer + 1).start()

            @pl.when(t == first + per)
            def _():
                load(2 * layer + 1).wait()
                if layer + 1 < layers:
                    load(2 * layer + 2).start()

            @pl.when((t >= first) & (t < first + per))
            def _():
                o = dot(x_refs[2 * layer][...].reshape(4 * ROWS, tokens), right[0], NN)
                for q in range(4):
                    acc[t % 2, q] = o[ROWS * q : ROWS * (q + 1)]

            @pl.when((t >= first + per) & (t < first + 3 * per))
            def _():
                o = dot(x_refs[2 * layer + 1][...], right[1], NN)
                for q in range(4):
                    for p in range(4):
                        acc[t % 2, p, :, wide * q : wide * (q + 1)] = o[ROWS * q : ROWS * (q + 1), wide * p : wide * (p + 1)]

        @pl.when(t >= LAG[4])
        def _():
            u = t - LAG[4]
            along_z(u).wait()
            out[0] = (zsend[u % slots].astype(F32) + zrecv[u % slots].astype(F32)).astype(BF)

        @pl.when((t >= LAG[3]) & (t < chunks + LAG[3]))
        def _():
            u = t - LAG[3]
            along_y(u).wait()
            zsend[u % slots] = (ysend[u % slots].astype(F32) + yrecv[u % slots].astype(F32)).astype(BF)
            along_z(u).start()

        @pl.when((t >= LAG[2]) & (t < chunks + LAG[2]))
        def _():
            u = t - LAG[2]
            along_x(u).wait()
            ysend[u % slots] = (mine[u % slots] + xrecv[u % slots].astype(F32)).astype(BF)
            along_y(u).start()

        @pl.when((t >= LAG[1]) & (t < chunks + LAG[1]))
        def _():
            u = t - LAG[1]
            along_core(u).wait()
            xsend[u % slots] = (acc[u % 2, 2 - 2 * x + core] + crecv[u % 2, 1 - x].astype(F32)).astype(BF)
            along_x(u).start()
            mine[u % slots] = acc[u % 2, 2 * x + core] + crecv[u % 2, x].astype(F32)

        @pl.when(t < chunks)
        def _():
            for j in range(2):
                csend[t % 2, j] = acc[t % 2, 2 * j + 1 - core].astype(BF)
            along_core(t).start()

    def lhs(layer):
        def pieces(t):
            return 0, 0, jnp.clip(t - layer * 3 * per, 0, per - 1), 0

        def rows(t):
            u = jnp.clip(t - layer * 3 * per - per, 0, 2 * per - 1)
            return 1 + u // per, u % per, 0

        return [pl.BlockSpec((None, 4, ROWS, tokens), pieces), pl.BlockSpec((None, 4 * ROWS, tokens), rows)]

    block = (ROWS, d)
    dma = pltpu.SemaphoreType.DMA
    return pl.pallas_call(
        kernel,
        out_shape=jax.ShapeDtypeStruct((chunks,) + block, BF),
        grid=(chunks + LAG[4],),
        in_specs=[spec for layer in range(layers) for spec in lhs(layer)] + [pl.BlockSpec(memory_space=pl.ANY)] * (2 * layers),
        out_specs=pl.BlockSpec((1,) + block, lambda t: (jnp.maximum(t - LAG[4], 0), 0, 0)),
        scratch_shapes=[
            pltpu.VMEM((2, tokens, d), BF),
            pltpu.VMEM((2, 4) + block, F32),
            pltpu.VMEM((2, 2) + block, BF),
            pltpu.VMEM((2, 2) + block, BF),
            pltpu.VMEM((slots,) + block, F32),
        ]
        + [pltpu.VMEM((slots,) + block, BF)] * 6
        + [dma((2,)), dma((2, 2)), dma((2, slots)), dma((2, slots)), dma((2, slots))],
        compiler_params=params(1, collective_id=0, has_side_effects=True),
        cost_estimate=cost(2 * chunks * 4 * ROWS * tokens * d, 2 * layers * tokens * (3 * n + 2 * d)),
        name="summed",
    )(*[view for x in xs for view in (x.reshape(3, 4, quarter, tokens), x)], *[r for pair in rights for r in pair])


def stepped(g, weights, ms, vs):
    layers, quarter, d = weights[2].shape
    per = quarter // ROWS
    wide = d // 4

    def kernel(*refs):
        for j in range(3):
            g = refs[j][...].astype(F32)
            if j < 2:
                g = jnp.concatenate([g[:, wide * q : wide * (q + 1)] for q in range(4)], axis=0).T
            new = adamw(refs[3 + j][...].astype(F32), refs[6 + j][...], refs[9 + j][...], g)
            for which in range(3):
                refs[12 + 3 * which + j][...] = new[which]

    def chunk(j):
        return pl.BlockSpec((None, ROWS, d), lambda l, k: ((layers - 1 - l) * 3 * per + j * per + k, 0, 0))

    column = pl.BlockSpec((None, wide, 4 * ROWS), lambda l, k: (l, 0, k))
    blocks = [column, column, pl.BlockSpec((None, ROWS, d), lambda l, k: (l, k, 0))]
    return pl.pallas_call(
        kernel,
        out_shape=tuple(jax.ShapeDtypeStruct(a.shape, a.dtype) for a in (*weights, *ms, *vs)),
        grid=(layers, per),
        in_specs=[chunk(1), chunk(2), chunk(0)] + blocks * 3,
        out_specs=tuple(blocks * 3),
        compiler_params=params(2),
        cost_estimate=cost(20 * layers * 3 * quarter * d, 22 * layers * 3 * quarter * d),
        name="stepped",
    )(g, g, g, *weights, *ms, *vs)


def solution(mesh):
    def step(x, dy, *arrays):
        weights, m, v = (arrays[i : i + 3] for i in (0, 3, 6))
        layers, quarter, d = weights[2].shape
        h = x[0]
        *ps, a, gate, up, wd0 = started(h, *weights)
        kept = [(h, a)]
        h, a, wd1 = down(ps, wd0.reshape(4 * quarter, d), h, weights[2])
        kept.append((h, a))
        by_h = dy[0]
        xs, rights = [], []
        for number in reversed(range(layers)):
            h, a = kept[number]
            xs.append(inner(a, by_h, gate, up, (wd0, wd1)[number].reshape(4 * quarter, d), number))
            rights.append((by_h, a))
            if number:
                by_h = below(xs[-1], gate, up, number, h, by_h)
        return stepped(summed(xs, rights), weights, m, v)

    states, cut = P(("rep", "r", "s"), None, None), P(None, "s", None)
    return jax.shard_map(
        step,
        mesh=mesh,
        in_specs=(states, states) + (cut,) * 9,
        out_specs=(P("rep", "s", None),) * 9,
        check_vma=False,
    )
```

```python
import functools

import jax
import jax.numpy as jnp
from jax import lax
from jax.experimental import pallas as pl
from jax.experimental.pallas import tpu as pltpu
from jax.sharding import PartitionSpec as P

NAMES = ("w_gate", "w_up", "w_down")
BF, F32 = jnp.bfloat16, jnp.float32
MESH = pl.DeviceIdType.MESH
NN, TB, TA = ((((1,), (0,)), ((), ())), (((1,), (1,)), ((), ())), (((0,), (0,)), ((), ())))
VMEM = 60 * 2**20


def dot(a, b, dims):
    return lax.dot_general(a, b, dims, preferred_element_type=F32)


def whole(w):
    return jnp.concatenate([w[s] for s in range(4)], axis=1)


def scale_of(wide):
    return lax.rsqrt(jnp.mean(wide * wide, -1, keepdims=True) + 1e-6)


def normed(h):
    wide = h.astype(F32)
    return (wide * scale_of(wide)).astype(BF)


def adamw(w, m, v, g):
    m = 0.9 * m + 0.1 * g
    v = 0.95 * v + 0.05 * g * g
    step = m * lax.rsqrt(v + 1e-8) + 0.1 * w
    return (w - 0.02 * step).astype(BF), m, v


def params(axes, **more):
    return pltpu.CompilerParams(dimension_semantics=("arbitrary",) * axes, vmem_limit_bytes=VMEM, **more)


def cost(flops, bytes_):
    return pl.CostEstimate(flops=flops, bytes_accessed=bytes_, transcendentals=0)


def routes(sems):
    s, r = lax.axis_index("s"), lax.axis_index("r")
    core, px, py, pz = s % 2, s // 2, r // 2, r % 2
    sx = s + 2 - 4 * px
    to_core, to_x = {"s": s + 1 - 2 * core}, {"s": sx}
    to_y, to_z = {"r": r + 2 - 4 * py}, {"r": r + 1 - 2 * pz}

    def item(number, own, full, base, size, by):
        def copy(kind, src, dst, to):
            return pltpu.make_async_remote_copy(
                src_ref=src, dst_ref=dst, send_sem=sems.at[0, number, kind], recv_sem=sems.at[1, number, kind],
                device_id=to, device_id_type=MESH,
            )

        def relay(kind, rows, to):
            return copy(kind, full(sx, rows), full(sx, rows), to)

        every = pl.ds(base, size)
        if by in ("y", "z"):
            half = size // 2
            par = py if by == "y" else pz
            mine, theirs = pl.ds(base + par * half, half), pl.ds(base + (1 - par) * half, half)
            out = {
                "x": copy(0, own(mine), full(s, mine), to_x),
                "r": relay(2, mine, to_y if by == "y" else to_z),
                "cx": relay(3, mine, to_core),
                "cr": relay(4, theirs, to_core),
            }
        else:
            part = size // 4

            def at(y, z):
                return pl.ds(base + (2 * y + z) * part, part)

            mine = at(py, pz)
            out = {
                "x": copy(0, own(mine), full(s, mine), to_x),
                "y": relay(2, mine, to_y),
                "z": relay(3, mine, to_z),
                "cx": relay(4, mine, to_core),
                "cy": relay(5, at(1 - py, pz), to_core),
                "cz": relay(6, at(py, 1 - pz), to_core),
                "d": relay(7, at(1 - py, pz), to_z) if by == "yz" else relay(7, at(py, 1 - pz), to_y),
                "cd": relay(8, at(1 - py, 1 - pz), to_core),
            }
        out["c"] = copy(1, own(every), full(s, every), to_core)
        return out

    return item, s, (to_core, to_x, to_y, to_z)


def greet(partners):
    barrier = pltpu.get_barrier_semaphore()
    for to in partners:
        pl.semaphore_signal(barrier, inc=1, device_id=to, device_id_type=MESH)
    pl.semaphore_wait(barrier, len(partners))


def got(one, *kinds):
    for kind in kinds:
        one[kind].wait_recv()


def go(one, *kinds):
    for kind in kinds:
        one[kind].start()


FOUR = ("c", "cx", "cy", "cz", "cd")
TILES = (512, 896, 1408)


def started(x, w_gate, w_up, w_down, tm=512):
    tokens, d = x.shape
    layers, wide, n = w_gate.shape
    quarter = n // 4
    steps_m = tokens // tm
    bases = tuple(sum(TILES[:i]) for i in range(len(TILES)))
    last = len(TILES) * steps_m

    def kernel(x_ref, g_ref, u_ref, d_ref, p0, p1, p2, a_ref, fg, fu, fd, a, g0, u0, turned, flat, dv, sems, local):
        t = pl.program_id(0)
        item, s, partners = routes(sems)

        def inside(ref):
            return (lambda rows: ref.at[s, rows]), (lambda block, rows: ref.at[block, rows])

        def outside(own, ref):
            return (lambda rows: own.at[rows]), (lambda block, rows: ref.at[1, block, rows])

        tiles = [
            (item(2 * i, *inside(g0), bases[i], TILES[i], "y"), item(2 * i + 1, *inside(u0), bases[i], TILES[i], "z"))
            for i in range(len(TILES))
        ]
        d0 = item(6, lambda rows: d_ref.at[0, rows], lambda block, rows: fd.at[block, rows], 0, quarter, "yz")
        half = n // 2
        g1a, u1a = item(7, *outside(turned.at[0], fg), 0, half, "zy"), item(8, *outside(turned.at[1], fu), 0, half, "yz")
        g1b, u1b = item(9, *outside(turned.at[0], fg), half, half, "zy"), item(10, *outside(turned.at[1], fu), half, half, "yz")
        late = (d0, g1a, u1a, g1b, u1b)

        def here(k, src, dst):
            return pltpu.make_async_copy(src, dst, local.at[k])

        loads = [here(2 * i + j, ref.at[i], flat.at[2 * i + j]) for i in range(2) for j, ref in enumerate((g_ref, u_ref))]
        load_x, load_d = here(4, x_ref, a), here(5, d_ref.at[0], dv)
        keep = [
            here(6, turned.at[0], fg.at[1, s]),
            here(7, turned.at[1], fu.at[1, s]),
            here(8, dv, fd.at[s]),
            here(9, a, a_ref),
            here(10, g0, fg.at[0]),
            here(11, u0, fu.at[0]),
        ]

        @pl.when(t == 0)
        def _():
            for load in (*loads[:2], load_x, load_d, *loads[2:]):
                load.start()
            greet(partners)
            loads[0].wait()
            loads[1].wait()
            for base, size, pair in zip(bases, TILES, tiles, strict=True):
                for j, (ref, one) in enumerate(zip((g0, u0), pair, strict=True)):
                    ref[s, base : base + size] = flat[j, :, base : base + size].T
                    go(one, "x", "c")
            go(d0, "x", "c")
            load_x.wait()

            @pl.loop(0, steps_m)
            def _(i):
                rows = pl.ds(i * tm, tm)
                a[rows, :] = normed(a[rows, :])

            keep[3].start()
            g00, u00 = tiles[0]
            got(g00, "x")
            go(g00, "r", "cx")
            got(u00, "x")
            go(u00, "r", "cx")
            got(g00, "r")
            go(g00, "cr")
            got(u00, "r")
            go(u00, "cr")
            for j in range(2):
                loads[2 + j].wait()
                for base in (0, half):
                    turned[j, base : base + half] = flat[2 + j, :, base : base + half].T
                keep[j].start()
            for one in late[1:]:
                go(one, "x", "c")
            load_d.wait()
            keep[2].start()

        def on(step, *todo):
            @pl.when(t == step)
            def _():
                for one, wait, then in todo:
                    got(one, *wait)
                    go(one, *then)

        (_, _), (g01, u01), (g02, u02) = tiles
        first, second, third = (("x",), ("y", "z", "cx")), (("y", "z"), ("cy", "cz", "d")), (("d",), ("cd",))
        near, far = (("x",), ("r", "cx")), (("r",), ("cr",))
        on(1, (g01, *near))
        on(3, (u01, *near))
        on(6, (g01, *far))
        on(8, (u01, *far), (g02, *near))
        on(11, (u02, *near))
        on(12, (g02, *far))
        on(14, (d0, *first))
        on(16, (u02, *far), (g1a, *first))
        on(17, (u1a, *first))
        on(18, (d0, *second), (g1b, *first))
        on(19, (g1a, *second), (u1b, *first))
        on(20, (u1a, *second))
        on(21, (g1b, *second), (d0, *third))
        on(22, (u1b, *second), (g1a, *third))
        on(23, (u1a, *third))

        for i, (base, size, pair, p_ref) in enumerate(zip(bases, TILES, tiles, (p0, p1, p2), strict=True)):

            @pl.when(t == i * steps_m)
            def _():
                for one in pair:
                    got(one, "c", "cx", "cr")
                if i == len(TILES) - 1:
                    keep[4].start()
                    keep[5].start()

            @pl.when((t >= i * steps_m) & (t < (i + 1) * steps_m))
            def _():
                block = a[pl.ds((t - i * steps_m) * tm, tm), :]
                gate = dot(block, whole([g0[q, base : base + size] for q in range(4)]), TB)
                up = dot(block, whole([u0[q, base : base + size] for q in range(4)]), TB)
                p_ref[...] = (gate * jax.nn.sigmoid(gate) * up).astype(BF)

        @pl.when(t == last - 1)
        def _():
            for one in (g1b, u1b):
                got(one, "d")
                go(one, "cd")
            for one in late:
                got(one, *FOUR)
            for one in (*[one for pair in tiles for one in pair], *late):
                for copy in one.values():
                    copy.wait_send()
            for copy in keep:
                copy.wait()

    def part(i):
        return pl.BlockSpec((tm, TILES[i]), lambda t: (jnp.clip(t - i * steps_m, 0, steps_m - 1), 0))

    hbm = pl.BlockSpec(memory_space=pl.ANY)
    dma = pltpu.SemaphoreType.DMA
    full = jax.ShapeDtypeStruct((layers, 4, n, wide), BF)
    return pl.pallas_call(
        kernel,
        out_shape=(
            *[jax.ShapeDtypeStruct((tokens, size), BF) for size in TILES],
            jax.ShapeDtypeStruct((tokens, d), BF),
            full,
            full,
            jax.ShapeDtypeStruct((4, quarter, d), BF),
        ),
        grid=(last,),
        in_specs=[hbm] * 4,
        out_specs=(*[part(i) for i in range(len(TILES))], hbm, hbm, hbm, hbm),
        scratch_shapes=[
            pltpu.VMEM((tokens, d), BF),
            pltpu.VMEM((4, n, wide), BF),
            pltpu.VMEM((4, n, wide), BF),
            pltpu.VMEM((2, n, wide), BF),
            pltpu.VMEM((4, wide, n), BF),
            pltpu.VMEM((quarter, d), BF),
            dma((2, 11, 9)),
            dma((12,)),
        ],
        compiler_params=params(1, collective_id=1, has_side_effects=True),
        cost_estimate=cost(4 * tokens * d * n, 2 * tokens * (d + n)),
        name="started",
    )(x, w_gate, w_up, w_down)


def down(ps, wd, h, w_down, tm=512):
    tokens, d = h.shape
    n = wd.shape[0]
    quarter = n // 4
    steps = tokens // tm
    cut = 384

    def kernel(p0, p1, p2, w, h, d_ref, ho, ao, fd, dv, sems, local):
        t = pl.program_id(0)
        item, s, partners = routes(sems)

        def one(number, base, size, by):
            return item(number, lambda rows: d_ref.at[1, rows], lambda block, rows: fd.at[block, rows], base, size, by)

        a, b = one(0, 0, cut, "yz"), one(1, cut, quarter - cut, "zy")
        load = pltpu.make_async_copy(d_ref.at[1], dv, local.at[0])
        keep = pltpu.make_async_copy(dv, fd.at[s], local.at[1])

        @pl.when(t == 0)
        def _():
            load.start()
            greet(partners)
            for which in (a, b):
                go(which, "x", "c")
            load.wait()
            keep.start()

        for step, which, wait, then in (
            (2, a, ("x",), ("y", "z", "cx")),
            (3, b, ("x",), ("y", "z", "cx")),
            (4, a, ("y", "z"), ("cy", "cz", "d")),
            (5, b, ("y", "z"), ("cy", "cz", "d")),
            (6, a, ("d",), ("cd",)),
            (7, b, ("d",), ("cd",)),
        ):

            @pl.when(t == step)
            def _():
                got(which, *wait)
                go(which, *then)

        by_p = dot(jnp.concatenate([p0[...], p1[...], p2[...]], axis=1), w[...], NN)
        new = h[...] + by_p.astype(BF)
        ho[...] = new
        ao[...] = normed(new)

        @pl.when(t == steps - 1)
        def _():
            for which in (a, b):
                got(which, *FOUR)
                for copy in which.values():
                    copy.wait_send()
            keep.wait()

    row = pl.BlockSpec((tm, d), lambda m: (m, 0))
    hbm = pl.BlockSpec(memory_space=pl.ANY)
    dma = pltpu.SemaphoreType.DMA
    return pl.pallas_call(
        kernel,
        out_shape=(*[jax.ShapeDtypeStruct((tokens, d), BF)] * 2, jax.ShapeDtypeStruct((4, quarter, d), BF)),
        grid=(steps,),
        in_specs=[pl.BlockSpec((tm, size), lambda m: (m, 0)) for size in TILES] + [pl.BlockSpec((n, d), lambda m: (0, 0)), row, hbm],
        out_specs=(row, row, hbm),
        scratch_shapes=[pltpu.VMEM((quarter, d), BF), dma((2, 2, 9)), dma((2,))],
        compiler_params=params(1, collective_id=2, has_side_effects=True),
        cost_estimate=cost(2 * tokens * d * n, 2 * tokens * (3 * d + n)),
        name="down",
    )(*ps, wd, h, w_down)


def inner(a, dy, wg, wu, wd, layer, tm=1024, tn=704, lanes=256):
    tokens, d = a.shape
    n = wd.shape[0]

    def kernel(a, dy, g, u, w, o):
        to_gate, to_up = whole(g), whole(u)
        for start in range(0, tm, lanes):
            part = slice(start, start + lanes)
            gate, up = dot(to_gate, a[part], TB), dot(to_up, a[part], TB)
            by_p = dot(w[...], dy[part], TB).astype(BF).astype(F32)
            sig = 0.5 * jnp.tanh(0.5 * gate) + 0.5
            act = gate * sig
            o[0, :, part] = (act * up).astype(BF)
            o[1, :, part] = (by_p * up * (sig * (1.0 + gate * (1.0 - sig)))).astype(BF)
            o[2, :, part] = (by_p * act).astype(BF)

    w = pl.BlockSpec((None, 4, tn, d // 4), lambda n, m: (layer, 0, n, 0))
    act = pl.BlockSpec((tm, d), lambda n, m: (m, 0))
    return pl.pallas_call(
        kernel,
        out_shape=jax.ShapeDtypeStruct((3, n, tokens), BF),
        grid=(n // tn, tokens // tm),
        in_specs=[act, act, w, w, pl.BlockSpec((tn, d), lambda n, m: (n, 0))],
        out_specs=pl.BlockSpec((3, tn, tm), lambda n, m: (0, n, m)),
        compiler_params=params(2),
        cost_estimate=cost(6 * tokens * d * n, 2 * tokens * (2 * d + 3 * n)),
        name="inner",
    )(a, dy, wg, wu, wd)


def below(x, wg, wu, layer, h, dh, tm=256):
    tokens, d = h.shape
    n = x.shape[1]

    def kernel(x, g, u, h, dh, o):
        by_a = dot(x[0], whole(g), TA).astype(BF).astype(F32) + dot(x[1], whole(u), TA).astype(BF).astype(F32)
        wide = h[...].astype(F32)
        r = scale_of(wide)
        by_h = by_a * r - wide * (r * r * r) * jnp.mean(by_a * wide, -1, keepdims=True)
        o[...] = dh[...] + by_h.astype(BF)

    row = pl.BlockSpec((tm, d), lambda m: (m, 0))
    w = pl.BlockSpec((None, 4, n, d // 4), lambda m: (layer, 0, 0, 0))

    def two(x_gate, x_up, g, u, h, dh, o):
        kernel((x_gate[0], x_up[0]), g, u, h, dh, o)

    return pl.pallas_call(
        two,
        out_shape=jax.ShapeDtypeStruct((tokens, d), BF),
        grid=(tokens // tm,),
        in_specs=[pl.BlockSpec((1, n, tm), lambda m: (1, 0, m)), pl.BlockSpec((1, n, tm), lambda m: (2, 0, m)), w, w, row, row],
        out_specs=row,
        compiler_params=params(1),
        cost_estimate=cost(4 * tokens * d * n, 2 * tokens * (3 * d + 2 * n)),
        name="below",
    )(x, x, wg, wu, h, dh)


LAG = (0, 1, 3, 5, 7)
ROWS = 64


def summed(xs, rights):
    _, n, tokens = xs[0].shape
    d = rights[0][0].shape[1]
    quarter = n // 4
    per = quarter // ROWS
    layers = len(xs)
    chunks = layers * 3 * per
    wide = d // 4
    slots = 4

    def kernel(*refs):
        x_refs, r_refs = refs[: 2 * layers], refs[2 * layers : 4 * layers]
        out, right, acc, csend, crecv, mine, xsend, xrecv, ysend, yrecv, zsend, zrecv, rsem, csems, xsems, ysems, zsems = refs[4 * layers :]
        t = pl.program_id(0)
        s, r = lax.axis_index("s"), lax.axis_index("r")
        core, x, y, z = s % 2, s // 2, r // 2, r % 2
        other, over_x, over_y, over_z = s + 1 - 2 * core, s + 2 - 4 * x, r + 2 - 4 * y, r + 1 - 2 * z

        def load(i):
            return pltpu.make_async_copy(r_refs[i], right.at[i % 2], rsem.at[i % 2])

        def send(src, dst, sems, slot, to):
            return pltpu.make_async_remote_copy(
                src_ref=src.at[slot], dst_ref=dst.at[slot], send_sem=sems.at[0, slot], recv_sem=sems.at[1, slot],
                device_id=to, device_id_type=MESH,
            )

        def along_core(u):
            return send(csend, crecv, csems, u % 2, {"s": other})

        def along_x(u):
            return send(xsend, xrecv, xsems, u % slots, {"s": over_x})

        def along_y(u):
            return send(ysend, yrecv, ysems, u % slots, {"r": over_y})

        def along_z(u):
            return send(zsend, zrecv, zsems, u % slots, {"r": over_z})

        @pl.when(t == 0)
        def _():
            load(0).start()
            barrier = pltpu.get_barrier_semaphore()
            for to in ({"s": other}, {"s": over_x}, {"r": over_y}, {"r": over_z}):
                pl.semaphore_signal(barrier, inc=1, device_id=to, device_id_type=MESH)
            pl.semaphore_wait(barrier, 4)

        for layer in range(layers):
            first = layer * 3 * per

            @pl.when(t == first)
            def _():
                load(2 * layer).wait()
                load(2 * layer + 1).start()

            @pl.when(t == first + per)
            def _():
                load(2 * layer + 1).wait()
                if layer + 1 < layers:
                    load(2 * layer + 2).start()

            @pl.when((t >= first) & (t < first + per))
            def _():
                o = dot(x_refs[2 * layer][...].reshape(4 * ROWS, tokens), right[0], NN)
                for q in range(4):
                    acc[t % 2, q] = o[ROWS * q : ROWS * (q + 1)]

            @pl.when((t >= first + per) & (t < first + 3 * per))
            def _():
                o = dot(x_refs[2 * layer + 1][...], right[1], NN)
                for q in range(4):
                    for p in range(4):
                        acc[t % 2, p, :, wide * q : wide * (q + 1)] = o[ROWS * q : ROWS * (q + 1), wide * p : wide * (p + 1)]

        @pl.when(t >= LAG[4])
        def _():
            u = t - LAG[4]
            along_z(u).wait()
            out[0] = (zsend[u % slots].astype(F32) + zrecv[u % slots].astype(F32)).astype(BF)

        @pl.when((t >= LAG[3]) & (t < chunks + LAG[3]))
        def _():
            u = t - LAG[3]
            along_y(u).wait()
            zsend[u % slots] = (ysend[u % slots].astype(F32) + yrecv[u % slots].astype(F32)).astype(BF)
            along_z(u).start()

        @pl.when((t >= LAG[2]) & (t < chunks + LAG[2]))
        def _():
            u = t - LAG[2]
            along_x(u).wait()
            ysend[u % slots] = (mine[u % slots] + xrecv[u % slots].astype(F32)).astype(BF)
            along_y(u).start()

        @pl.when((t >= LAG[1]) & (t < chunks + LAG[1]))
        def _():
            u = t - LAG[1]
            along_core(u).wait()
            xsend[u % slots] = (acc[u % 2, 2 - 2 * x + core] + crecv[u % 2, 1 - x].astype(F32)).astype(BF)
            along_x(u).start()
            mine[u % slots] = acc[u % 2, 2 * x + core] + crecv[u % 2, x].astype(F32)

        @pl.when(t < chunks)
        def _():
            for j in range(2):
                csend[t % 2, j] = acc[t % 2, 2 * j + 1 - core].astype(BF)
            along_core(t).start()

    def lhs(layer):
        def pieces(t):
            return 0, 0, jnp.clip(t - layer * 3 * per, 0, per - 1), 0

        def rows(t):
            u = jnp.clip(t - layer * 3 * per - per, 0, 2 * per - 1)
            return 1 + u // per, u % per, 0

        return [pl.BlockSpec((None, 4, ROWS, tokens), pieces), pl.BlockSpec((None, 4 * ROWS, tokens), rows)]

    block = (ROWS, d)
    dma = pltpu.SemaphoreType.DMA
    return pl.pallas_call(
        kernel,
        out_shape=jax.ShapeDtypeStruct((chunks,) + block, BF),
        grid=(chunks + LAG[4],),
        in_specs=[spec for layer in range(layers) for spec in lhs(layer)] + [pl.BlockSpec(memory_space=pl.ANY)] * (2 * layers),
        out_specs=pl.BlockSpec((1,) + block, lambda t: (jnp.maximum(t - LAG[4], 0), 0, 0)),
        scratch_shapes=[
            pltpu.VMEM((2, tokens, d), BF),
            pltpu.VMEM((2, 4) + block, F32),
            pltpu.VMEM((2, 2) + block, BF),
            pltpu.VMEM((2, 2) + block, BF),
            pltpu.VMEM((slots,) + block, F32),
        ]
        + [pltpu.VMEM((slots,) + block, BF)] * 6
        + [dma((2,)), dma((2, 2)), dma((2, slots)), dma((2, slots)), dma((2, slots))],
        compiler_params=params(1, collective_id=0, has_side_effects=True),
        cost_estimate=cost(2 * chunks * 4 * ROWS * tokens * d, 2 * layers * tokens * (3 * n + 2 * d)),
        name="summed",
    )(*[view for x in xs for view in (x.reshape(3, 4, quarter, tokens), x)], *[r for pair in rights for r in pair])


def stepped(g, weights, ms, vs):
    layers, quarter, d = weights[2].shape
    per = quarter // ROWS
    wide = d // 4

    def kernel(*refs):
        for j in range(3):
            g = refs[j][...].astype(F32)
            if j < 2:
                g = jnp.concatenate([g[:, wide * q : wide * (q + 1)] for q in range(4)], axis=0).T
            new = adamw(refs[3 + j][...].astype(F32), refs[6 + j][...], refs[9 + j][...], g)
            for which in range(3):
                refs[12 + 3 * which + j][...] = new[which]

    def chunk(j):
        return pl.BlockSpec((None, ROWS, d), lambda l, k: ((layers - 1 - l) * 3 * per + j * per + k, 0, 0))

    column = pl.BlockSpec((None, wide, 4 * ROWS), lambda l, k: (l, 0, k))
    blocks = [column, column, pl.BlockSpec((None, ROWS, d), lambda l, k: (l, k, 0))]
    return pl.pallas_call(
        kernel,
        out_shape=tuple(jax.ShapeDtypeStruct(a.shape, a.dtype) for a in (*weights, *ms, *vs)),
        grid=(layers, per),
        in_specs=[chunk(1), chunk(2), chunk(0)] + blocks * 3,
        out_specs=tuple(blocks * 3),
        compiler_params=params(2),
        cost_estimate=cost(20 * layers * 3 * quarter * d, 22 * layers * 3 * quarter * d),
        name="stepped",
    )(g, g, g, *weights, *ms, *vs)


def solution(mesh):
    def step(x, dy, *arrays):
        weights, m, v = (arrays[i : i + 3] for i in (0, 3, 6))
        layers, quarter, d = weights[2].shape
        h = x[0]
        *ps, a, gate, up, wd0 = started(h, *weights)
        kept = [(h, a)]
        h, a, wd1 = down(ps, wd0.reshape(4 * quarter, d), h, weights[2])
        kept.append((h, a))
        by_h = dy[0]
        xs, rights = [], []
        for number in reversed(range(layers)):
            h, a = kept[number]
            xs.append(inner(a, by_h, gate, up, (wd0, wd1)[number].reshape(4 * quarter, d), number))
            rights.append((by_h, a))
            if number:
                by_h = below(xs[-1], gate, up, number, h, by_h)
        return stepped(summed(xs, rights), weights, m, v)

    states, cut = P(("rep", "r", "s"), None, None), P(None, "s", None)
    return jax.shard_map(
        step,
        mesh=mesh,
        in_specs=(states, states) + (cut,) * 9,
        out_specs=(P("rep", "s", None),) * 9,
        check_vma=False,
    )
```
